32 devices in a mesh: dp: 1 (over z), ep: 32 (over y, x, core).
Axes of the slice: x: 4, y: 4, z: 1, core: 2. Of those that a mesh axis runs over, the one named last changes fastest.
The devices are a block of a 4x4x8 slice.
Arguments:
- hidden: bfloat16 [32768, 2048], P(('dp', 'ep'))
- w_router: bfloat16 [2048, 64], replicated
- w_gate: bfloat16 [64, 2048, 1408], P('ep')
- w_up: bfloat16 [64, 2048, 1408], P('ep')
- w_down: bfloat16 [64, 1408, 2048], P('ep')
- shared_gate: bfloat16 [2048, 2816], replicated
- shared_up: bfloat16 [2048, 2816], replicated
- shared_down: bfloat16 [2816, 2048], replicated
- top_idx: int32 [32768, 6], P(('dp', 'ep'))
- keep_mask: int32 [32768, 6], P(('dp', 'ep'))
Outputs:
- output: bfloat16 [32768, 2048], P(('dp', 'ep'))
All inputs are finite; a program needn't handle non-finite values.
Results may differ from the reference program's by a relative error of at most 0.00690417.
Values are sent between devices in bfloat16 or wider.
A program may use at most 768 MiB of HBM per device.

```python
import math
import jax
import jax.numpy as jnp
from jax import lax

HIDDEN = 2048
EXPERTS = 64
EXPERT_FF = 1408
SHARED_FF = 2816
TOP_K = 6
DEV_LIMIT = 6
TOKENS = 1024
GROUP_SIZE = 32
CAPACITY = 192

ROUTE_SCALE = 16.0
PER_DEVICE = EXPERTS // GROUP_SIZE
PART_TOKENS = GROUP_SIZE * TOKENS
ROUTED_GAIN = EXPERTS / (ROUTE_SCALE * math.sqrt(TOP_K))


def draw_routing(route_key):
    k_noise, k_dev, k_exp, k_hot = jax.random.split(route_key, 4)
    expert_ids = jnp.arange(EXPERTS, dtype=jnp.int32)
    noise_int = jax.random.randint(k_noise, (PART_TOKENS, EXPERTS), 0, 256, dtype=jnp.int32)
    dev_bias = jax.random.randint(k_dev, (GROUP_SIZE,), 0, 128, dtype=jnp.int32)
    exp_bias = jax.random.randint(k_exp, (EXPERTS,), 0, 64, dtype=jnp.int32)
    hot_expert = jax.random.randint(k_hot, (), 0, EXPERTS, dtype=jnp.int32)
    bias_all = exp_bias + jnp.repeat(dev_bias, PER_DEVICE) + jnp.where(expert_ids == hot_expert, 1024, 0)
    pair_score = (noise_int + bias_all[None, :]) * EXPERTS + expert_ids[None, :]
    dev_score = jnp.max(pair_score.reshape(PART_TOKENS, GROUP_SIZE, PER_DEVICE), axis=2)
    top_dev = lax.top_k(dev_score, DEV_LIMIT)[1]
    chosen = jnp.any(top_dev[:, :, None] == jnp.arange(GROUP_SIZE, dtype=jnp.int32)[None, None, :], axis=1)
    masked = jnp.where(jnp.repeat(chosen, PER_DEVICE, axis=1), pair_score, -1)
    top_idx = lax.top_k(masked, TOP_K)[1].astype(jnp.int32)

    def rank_pairs(src_pairs):
        onehot = (src_pairs[:, None] == expert_ids[None, :]).astype(jnp.int32)
        return jnp.sum((jnp.cumsum(onehot, axis=0) - 1) * onehot, axis=1)

    pair_rank = lax.map(rank_pairs, top_idx.reshape(GROUP_SIZE, TOKENS * TOP_K))
    keep_mask = (pair_rank < CAPACITY).astype(jnp.int32).reshape(PART_TOKENS, TOP_K)
    return top_idx, keep_mask


def draw_bank(bank_key, mat_shape, std_scale):
    key_list = jax.random.split(bank_key, EXPERTS)
    return lax.map(lambda one_key: (jax.random.normal(one_key, mat_shape, jnp.float32) * std_scale).astype(jnp.bfloat16), key_list)


def draw_matrix(mat_key, mat_shape, std_scale):
    return (jax.random.normal(mat_key, mat_shape, jnp.float32) * std_scale).astype(jnp.bfloat16)


def setup_inputs(seed: int = 0, part: int = 0) -> dict:
    root_key = jax.random.key(seed)
    part_key = jax.random.fold_in(root_key, part)
    k_hidden, k_route = jax.random.split(part_key, 2)
    k_router, k_gate, k_up, k_down, k_sgate, k_sup, k_sdown = jax.random.split(root_key, 7)
    top_idx, keep_mask = draw_routing(k_route)
    in_scale = HIDDEN ** -0.5
    return {
        "hidden": draw_matrix(k_hidden, (PART_TOKENS, HIDDEN), 1.0),
        "w_router": draw_matrix(k_router, (HIDDEN, EXPERTS), 0.5 * in_scale),
        "w_gate": draw_bank(k_gate, (HIDDEN, EXPERT_FF), in_scale),
        "w_up": draw_bank(k_up, (HIDDEN, EXPERT_FF), in_scale),
        "w_down": draw_bank(k_down, (EXPERT_FF, HIDDEN), ROUTED_GAIN * EXPERT_FF ** -0.5),
        "shared_gate": draw_matrix(k_sgate, (HIDDEN, SHARED_FF), in_scale),
        "shared_up": draw_matrix(k_sup, (HIDDEN, SHARED_FF), in_scale),
        "shared_down": draw_matrix(k_sdown, (SHARED_FF, HIDDEN), SHARED_FF ** -0.5),
        "top_idx": top_idx,
        "keep_mask": keep_mask,
    }


def swiglu(tok_rows, gate_w, up_w, down_w):
    h_gate = jnp.dot(tok_rows, gate_w, preferred_element_type=jnp.float32)
    h_up = jnp.dot(tok_rows, up_w, preferred_element_type=jnp.float32)
    act_rows = (jax.nn.silu(h_gate) * h_up).astype(jnp.bfloat16)
    return jnp.dot(act_rows, down_w, preferred_element_type=jnp.float32)


def reference(hidden, w_router, w_gate, w_up, w_down, shared_gate, shared_up, shared_down, top_idx, keep_mask):
    logits = jnp.dot(hidden, w_router, preferred_element_type=jnp.float32)
    router_prob = jax.nn.softmax(logits, axis=-1)
    gate_vals = ROUTE_SCALE * jnp.take_along_axis(router_prob, top_idx, axis=1) * keep_mask.astype(jnp.float32)
    pair_expert = top_idx.reshape(-1)
    pair_kept = keep_mask.reshape(-1) > 0
    pair_gate = gate_vals.reshape(-1)
    pair_token = jnp.arange(PART_TOKENS * TOP_K, dtype=jnp.int32) // TOP_K
    max_rows = GROUP_SIZE * CAPACITY

    def expert_step(routed_acc, per_expert):
        gate_w, up_w, down_w, expert_id = per_expert
        member = pair_kept & (pair_expert == expert_id)
        pair_slot = jnp.where(member, jnp.cumsum(member.astype(jnp.int32)) - 1, max_rows)
        row_token = jnp.zeros((max_rows,), jnp.int32).at[pair_slot].set(pair_token, mode="drop")
        row_gate = jnp.zeros((max_rows,), jnp.float32).at[pair_slot].set(pair_gate, mode="drop")
        expert_out = swiglu(hidden[row_token], gate_w, up_w, down_w).astype(jnp.bfloat16)
        routed_acc = routed_acc.at[row_token].add(row_gate[:, None] * expert_out.astype(jnp.float32))
        return routed_acc, None

    routed = lax.scan(expert_step, jnp.zeros((PART_TOKENS, HIDDEN), jnp.float32), (w_gate, w_up, w_down, jnp.arange(EXPERTS, dtype=jnp.int32)))[0]
    shared = lax.map(lambda tok_block: swiglu(tok_block, shared_gate, shared_up, shared_down), hidden.reshape(GROUP_SIZE, TOKENS, HIDDEN)).reshape(PART_TOKENS, HIDDEN)
    return (shared + routed).astype(jnp.bfloat16)
```

```python
import functools

import jax
import jax.numpy as jnp
from jax import lax
from jax.experimental import pallas as pl
from jax.experimental.pallas import tpu as pltpu
from jax.sharding import PartitionSpec as P

ROUTE_SCALE = 16.0
GROUP_BLOCKS = 4
COL = 256
VMEM_LIMIT = 63 * 1024 * 1024


def swiglu(tok_rows, gate_w, up_w, down_w):
    h_gate = jnp.dot(tok_rows, gate_w, preferred_element_type=jnp.float32)
    h_up = jnp.dot(tok_rows, up_w, preferred_element_type=jnp.float32)
    act_rows = (jax.nn.silu(h_gate) * h_up).astype(jnp.bfloat16)
    return jnp.dot(act_rows, down_w, preferred_element_type=jnp.float32)


def dot32(a, b):
    return jnp.dot(a, b, preferred_element_type=jnp.float32)


def expert_kernel(which, cap, tab_ref, x_ref, w1_ref, w3_ref, w2_ref, o_ref, rows, gates, act, tail):
    block = pl.program_id(0)
    slot = lax.rem(block, GROUP_BLOCKS)
    ff = w1_ref.shape[2]
    full = ff // COL * COL
    half = ff - full
    tokens = x_ref.shape[1]

    if half:
        @pl.when(block == 0)
        def _():
            tail[:, :half] = w1_ref[0, :, full:]
            tail[:, half:] = w3_ref[0, :, full:]

    per_dev = tab_ref.shape[1] // 2
    rank = tab_ref[0, which:which + 1, :].astype(jnp.int32)
    gate = tab_ref[0, per_dev + which:per_dev + which + 1, :]
    hit = rank == lax.broadcasted_iota(jnp.int32, (cap, tokens), 0)
    pick = jnp.where(hit, 1.0, 0.0).astype(jnp.bfloat16)
    at = pl.ds(pl.multiple_of(slot * cap, cap), cap)
    rows[at, :] = dot32(pick, x_ref[0]).astype(jnp.bfloat16)
    gates[at, :] = jnp.broadcast_to(jnp.sum(jnp.where(hit, gate, 0.0), axis=1, keepdims=True), (cap, 128))

    @pl.when(slot == GROUP_BLOCKS - 1)
    def _():
        tok = rows[...]
        for c in range(0, full, COL):
            h_gate = dot32(tok, w1_ref[0, :, c:c + COL])
            h_up = dot32(tok, w3_ref[0, :, c:c + COL])
            act[:, c:c + COL] = (jax.nn.silu(h_gate) * h_up).astype(jnp.bfloat16)
        if half:
            h_both = dot32(tok, tail[...])
            act[:, full:] = (jax.nn.silu(h_both[:, :half]) * h_both[:, half:]).astype(jnp.bfloat16)
        a = act[...]
        g = gates[:, :1]
        for c in range(0, w2_ref.shape[2], COL):
            e = dot32(a, w2_ref[0, :, c:c + COL]).astype(jnp.bfloat16).astype(jnp.float32)
            o_ref[:, :, c:c + COL] = (g * e).astype(jnp.bfloat16).reshape(GROUP_BLOCKS, cap, COL)


def expert_call(which, cap, tab, x_all, w1, w3, w2):
    blocks, tokens, dim = x_all.shape
    ff = w1.shape[2]
    once = pl.Buffered(1)
    rows = GROUP_BLOCKS * cap
    return pl.pallas_call(
        functools.partial(expert_kernel, which, cap),
        grid=(blocks,),
        in_specs=[
            pl.BlockSpec((1,) + tab.shape[1:], lambda b: (b, 0, 0)),
            pl.BlockSpec((1, tokens, dim), lambda b: (b, 0, 0)),
            pl.BlockSpec((1, dim, ff), lambda b: (which, 0, 0), pipeline_mode=once),
            pl.BlockSpec((1, dim, ff), lambda b: (which, 0, 0), pipeline_mode=once),
            pl.BlockSpec((1, ff, dim), lambda b: (which, 0, 0), pipeline_mode=once),
        ],
        out_specs=pl.BlockSpec((GROUP_BLOCKS, cap, dim), lambda b: (b // GROUP_BLOCKS, 0, 0)),
        out_shape=jax.ShapeDtypeStruct((blocks, cap, dim), jnp.bfloat16),
        scratch_shapes=[
            pltpu.VMEM((rows, dim), jnp.bfloat16),
            pltpu.VMEM((rows, 128), jnp.float32),
            pltpu.VMEM((rows, ff), jnp.bfloat16),
            pltpu.VMEM((dim, COL), jnp.bfloat16),
        ],
        compiler_params=pltpu.CompilerParams(dimension_semantics=("arbitrary",), vmem_limit_bytes=VMEM_LIMIT),
        cost_estimate=pl.CostEstimate(
            flops=2 * blocks * cap * dim * (3 * ff + tokens), bytes_accessed=2 * x_all.size, transcendentals=0),
        name=f"expert{which}",
    )(tab, x_all, w1, w3, w2)


def combine_kernel(cap, r_ref, back_ref, y_ref, o_ref, acc):
    step = pl.program_id(0)
    tokens, per = r_ref.shape[1], r_ref.shape[2]

    @pl.when(step == 0)
    def _():
        acc[...] = y_ref[...]

    ranks = r_ref[0]
    lanes = lax.broadcasted_iota(jnp.int32, (tokens, 128), 1)
    tiles = []
    for lo in range(0, per * cap, 128):
        hit = None
        for w in range(lo // cap, (lo + 127) // cap + 1):
            col = ranks[:, w:w + 1]
            now = jnp.where(col >= 0, col + (w * cap - lo), -1) == lanes
            hit = now if hit is None else hit | now
        tiles.append(jnp.where(hit, 1.0, 0.0).astype(jnp.bfloat16))
    pick = jnp.concatenate(tiles, axis=1)
    for c in range(0, acc.shape[1], 512):
        acc[:, c:c + 512] += dot32(pick, back_ref[0, :, c:c + 512])

    @pl.when(step == pl.num_programs(0) - 1)
    def _():
        o_ref[...] = acc[...].astype(o_ref.dtype)


def combine_call(cap, ranks, back, y, out_dtype):
    steps, tokens, per = ranks.shape
    dim = y.shape[1]
    return pl.pallas_call(
        functools.partial(combine_kernel, cap),
        grid=(steps,),
        in_specs=[
            pl.BlockSpec((1, tokens, per), lambda i: (i, 0, 0)),
            pl.BlockSpec((1, per * cap, dim), lambda i: (i, 0, 0)),
            pl.BlockSpec((tokens, dim), lambda i: (0, 0), pipeline_mode=pl.Buffered(1)),
        ],
        out_specs=pl.BlockSpec((tokens, dim), lambda i: (0, 0), pipeline_mode=pl.Buffered(1)),
        out_shape=jax.ShapeDtypeStruct((tokens, dim), out_dtype),
        scratch_shapes=[pltpu.VMEM((tokens, dim), jnp.float32)],
        compiler_params=pltpu.CompilerParams(dimension_semantics=("arbitrary",), vmem_limit_bytes=VMEM_LIMIT),
        cost_estimate=pl.CostEstimate(flops=2 * tokens * back.size, bytes_accessed=2 * back.size, transcendentals=0),
        name="combine",
    )(ranks, back.reshape(steps, per * cap, dim), y)


def routing(hidden, w_router, top_idx, keep_mask):
    experts = w_router.shape[1]
    tokens = hidden.shape[0]
    logits = jnp.dot(hidden, w_router, preferred_element_type=jnp.float32)
    prob = jax.nn.softmax(logits, axis=-1)
    chosen = (top_idx[:, :, None] == jnp.arange(experts)[None, None, :]) & (keep_mask[:, :, None] > 0)
    member = jnp.any(chosen, axis=1)
    lower = (jnp.arange(tokens)[:, None] >= jnp.arange(tokens)[None, :]).astype(jnp.bfloat16)
    count = jnp.dot(lower, member.astype(jnp.bfloat16), preferred_element_type=jnp.float32)
    rank = jnp.where(member, count - 1.0, -1.0)
    gate = jnp.where(member, ROUTE_SCALE * prob, 0.0)
    return rank, gate


def solution(mesh):
    groups = mesh.shape["ep"]
    tok_spec = P(("dp", "ep"), None)
    bank_spec = P("ep", None, None)

    def device_fn(hidden, w_router, w_gate, w_up, w_down, shared_gate, shared_up, shared_down, top_idx, keep_mask):
        tokens, top_k = top_idx.shape
        dim = hidden.shape[1]
        experts = w_router.shape[1]
        per_dev = w_gate.shape[0]
        cap = 8 * ((top_k * tokens + 4 * experts - 1) // (4 * experts))
        x_all = lax.all_gather(hidden, "ep", axis=0, tiled=True).reshape(groups, tokens, dim)
        rank, gate = routing(hidden, w_router, top_idx, keep_mask)
        table = jnp.concatenate([rank.T.reshape(groups, per_dev, tokens), gate.T.reshape(groups, per_dev, tokens)], axis=1)
        table = lax.all_to_all(table, "ep", 0, 0, tiled=True)
        y = swiglu(hidden, shared_gate, shared_up, shared_down)
        backs = []
        for which in range(per_dev):
            out = expert_call(which, cap, table, x_all, w_gate, w_up, w_down)
            backs.append(lax.all_to_all(out, "ep", 0, 0, tiled=True))
        per = 4
        for which in range(per_dev):
            ranks = rank[:, which::per_dev].astype(jnp.int32).reshape(tokens, groups // per, per).transpose(1, 0, 2)
            last = which == per_dev - 1
            y = combine_call(cap, ranks, backs[which], y, jnp.bfloat16 if last else jnp.float32)
        return y

    return jax.shard_map(device_fn, mesh=mesh, in_specs=(tok_spec, P(), bank_spec, bank_spec, bank_spec, P(), P(), P(), tok_spec, tok_spec), out_specs=tok_spec, check_vma=False)
```

```python
import functools
import math

import jax
import jax.numpy as jnp
from jax import lax
from jax.experimental import pallas as pl
from jax.experimental.pallas import tpu as pltpu
from jax.sharding import PartitionSpec as P

ROUTE_SCALE = 16.0
CORES = 2
COL = 256
VMEM_LIMIT = 63 * 1024 * 1024
MESH = pl.DeviceIdType.MESH


def swiglu(tok_rows, gate_w, up_w, down_w):
    h_gate = jnp.dot(tok_rows, gate_w, preferred_element_type=jnp.float32)
    h_up = jnp.dot(tok_rows, up_w, preferred_element_type=jnp.float32)
    act_rows = (jax.nn.silu(h_gate) * h_up).astype(jnp.bfloat16)
    return jnp.dot(act_rows, down_w, preferred_element_type=jnp.float32)


def dot32(a, b):
    return jnp.dot(a, b, preferred_element_type=jnp.float32)


def place(side):
    me = lax.axis_index("ep")
    return lax.rem(me // CORES, side), me // (CORES * side), lax.rem(me, CORES)


def device(side, x, y, k):
    return (lax.rem(y, side) * side + lax.rem(x, side)) * CORES + lax.rem(k, CORES)


def expert_kernel(side, cap, tab_ref, x_ref, w1_ref, w3_ref, w2_ref, recv, stage, xbuf, rows, act, tail, tile,
                  x_sem, stage_sem, send_a, recv_a, send_b, recv_b, self_sem):
    which, turn = pl.program_id(0), pl.program_id(1)
    turns = pl.num_programs(1)
    step = which * turns + turn
    steps = pl.num_programs(0) * turns
    ff = w1_ref.shape[2]
    full = ff // COL * COL
    rest = ff - full
    tokens, dim = x_ref.shape[1], x_ref.shape[2]
    half = dim // 2
    x, y, k = place(side)

    def offsets(s):
        i = lax.rem(s, turns)
        return s // turns, lax.rem(i // CORES + 1, side), lax.rem(i + 1, CORES)

    def fetch(s, j):
        _, dy, dc = offsets(s)
        return pltpu.make_async_copy(x_ref.at[device(side, x + j, y + dy, k + dc)], xbuf.at[j], x_sem.at[j])

    def to_column(s):
        e, dy, dc = offsets(s)
        return pltpu.make_async_remote_copy(
            src_ref=stage.at[s, 0], dst_ref=recv.at[0, y * CORES + k, e], send_sem=send_a.at[s], recv_sem=recv_a.at[s],
            device_id={"ep": device(side, x, y + dy, k + dc)}, device_id_type=MESH)

    def to_row(s, dx):
        e, dy, dc = offsets(s)
        return pltpu.make_async_remote_copy(
            src_ref=stage.at[s, 1, dx], dst_ref=recv.at[1, x * CORES + k, e, dy], send_sem=send_b.at[s, dx], recv_sem=recv_b.at[s, dx],
            device_id={"ep": device(side, x + dx, y, k + dc)}, device_id_type=MESH)

    def keep_column(s):
        e, _, _ = offsets(s)
        return pltpu.make_async_copy(tile.at[0], recv.at[0, y * CORES + k, e], self_sem.at[0])

    def keep_row(s):
        e, dy, _ = offsets(s)
        return pltpu.make_async_copy(tile.at[1, 0], recv.at[1, x * CORES + k, e, dy], self_sem.at[1])

    def put(s):
        return pltpu.make_async_copy(tile, stage.at[s], stage_sem)

    def remotes(s, act_on):
        _, dy, dc = offsets(s)

        @pl.when((dy != 0) | (dc != 0))
        def _():
            act_on(to_column(s))

        @pl.when(dc != 0)
        def _():
            act_on(to_row(s, 0))

        for dx in range(1, side):
            act_on(to_row(s, dx))

    def locals_(s, act_on):
        _, dy, dc = offsets(s)

        @pl.when((dy == 0) & (dc == 0))
        def _():
            act_on(keep_column(s))

        @pl.when(dc == 0)
        def _():
            act_on(keep_row(s))

    def flush(s):
        put(s).wait()
        locals_(s, lambda c: c.wait())
        remotes(s, lambda c: c.start())

    @pl.when(step == 0)
    def _():
        for j in range(side):
            fetch(0, j).start()

    if rest:
        @pl.when(turn == 0)
        def _():
            tail[:, :rest] = w1_ref[0, :, full:]
            tail[:, rest:] = w3_ref[0, :, full:]

    _, now_y, now_c = offsets(step)

    @pl.loop(0, side)
    def _(j):
        fetch(step, j).wait()
        rank = tab_ref[device(side, x + j, y + now_y, k + now_c), pl.ds(which, 1), :]
        hit = rank == lax.broadcasted_iota(jnp.int32, (cap, tokens), 0).astype(jnp.float32)
        pick = jnp.where(hit, 1.0, 0.0).astype(jnp.bfloat16)
        rows[pl.ds(pl.multiple_of(j * cap, cap), cap), :] = dot32(pick, xbuf[j]).astype(jnp.bfloat16)

        @pl.when(step + 1 < steps)
        def _():
            fetch(step + 1, j).start()

    @pl.when(step > 0)
    def _():
        flush(step - 1)

    tok = rows[...]
    for c in range(0, full, COL):
        h_gate = dot32(tok, w1_ref[0, :, c:c + COL])
        h_up = dot32(tok, w3_ref[0, :, c:c + COL])
        act[:, c:c + COL] = (jax.nn.silu(h_gate) * h_up).astype(jnp.bfloat16)
    if rest:
        h_both = dot32(tok, tail[...])
        act[:, full:] = (jax.nn.silu(h_both[:, :rest]) * h_both[:, rest:]).astype(jnp.bfloat16)
    a = act[...]
    for c in range(0, dim, COL):
        e = dot32(a, w2_ref[0, :, c:c + COL]).astype(jnp.bfloat16)
        at = c % half
        tile[c // half, :, :, at:at + COL] = e.reshape(side, cap, COL)

    put(step).start()
    locals_(step, lambda c: c.start())

    @pl.when(step == steps - 1)
    def _():
        flush(step)

        @pl.loop(0, steps)
        def _(s):
            remotes(s, lambda c: c.wait())


def expert_call(side, cap, tab, x_all, w1, w3, w2):
    blocks, tokens, dim = x_all.shape
    experts, _, ff = w1.shape
    once = pl.Buffered(1)
    turns = side * CORES
    steps = experts * turns
    rows = side * cap
    dma = pltpu.SemaphoreType.DMA
    recv, _ = pl.pallas_call(
        functools.partial(expert_kernel, side, cap),
        grid=(experts, turns),
        in_specs=[
            pl.BlockSpec(tab.shape, lambda e, t: (0, 0, 0), pipeline_mode=once),
            pl.BlockSpec(memory_space=pl.ANY),
            pl.BlockSpec((1, dim, ff), lambda e, t: (e, 0, 0), pipeline_mode=once),
            pl.BlockSpec((1, dim, ff), lambda e, t: (e, 0, 0), pipeline_mode=once),
            pl.BlockSpec((1, ff, dim), lambda e, t: (e, 0, 0), pipeline_mode=once),
        ],
        out_specs=[pl.BlockSpec(memory_space=pl.ANY)] * 2,
        out_shape=[
            jax.ShapeDtypeStruct((2, turns, experts, side, cap, dim // 2), jnp.bfloat16),
            jax.ShapeDtypeStruct((steps, 2, side, cap, dim // 2), jnp.bfloat16),
        ],
        scratch_shapes=[
            pltpu.VMEM((side, tokens, dim), jnp.bfloat16),
            pltpu.VMEM((rows, dim), jnp.bfloat16),
            pltpu.VMEM((rows, ff), jnp.bfloat16),
            pltpu.VMEM((dim, COL), jnp.bfloat16),
            pltpu.VMEM((2, side, cap, dim // 2), jnp.bfloat16),
            dma((side,)), dma, dma((steps,)), dma((steps,)), dma((steps, side)), dma((steps, side)), dma((2,)),
        ],
        compiler_params=pltpu.CompilerParams(
            dimension_semantics=("arbitrary", "arbitrary"), vmem_limit_bytes=VMEM_LIMIT, has_side_effects=True),
        cost_estimate=pl.CostEstimate(
            flops=2 * experts * blocks * cap * dim * (3 * ff + tokens), bytes_accessed=4 * x_all.size, transcendentals=0),
        name="experts",
    )(tab, x_all, w1, w3, w2)
    return recv


def combine_kernel(side, cap, t_ref, in_ref, recv, stage, pick, gate, acc, tile, stage_sem, send_sem, recv_sem, self_sem):
    turn, part = pl.program_id(0), pl.program_id(1)
    step = turn * 2 + part
    steps = 2 * side
    tokens = t_ref.shape[2]
    count = t_ref.shape[3] // 2
    experts = in_ref.shape[2]
    half = in_ref.shape[5]
    x, y, k = place(side)

    def offsets(s):
        return lax.rem(s // 2 + 1, side), lax.rem(s, 2)

    def send(s):
        rel, h = offsets(s)
        return pltpu.make_async_remote_copy(
            src_ref=stage.at[s], dst_ref=recv.at[h, rel], send_sem=send_sem.at[s], recv_sem=recv_sem.at[s],
            device_id={"ep": device(side, x + rel * (1 - h), y + rel * h, k)}, device_id_type=MESH)

    def put(s):
        return pltpu.make_async_copy(tile, stage.at[s], stage_sem)

    def keep(s):
        rel, h = offsets(s)
        return pltpu.make_async_copy(tile, recv.at[h, rel], self_sem)

    away = steps - 2

    @pl.when((step > 0) & (step <= away))
    def _():
        put(step - 1).wait()
        send(step - 1).start()

    @pl.when(step > away)
    def _():
        keep(step - 1).wait()

    lanes = lax.broadcasted_iota(jnp.int32, (tokens, cap), 1).astype(jnp.float32)
    for e in range(count):
        pick[e] = jnp.where(t_ref[0, 0, :, e:e + 1] == lanes, 1.0, 0.0).astype(jnp.bfloat16)
        gate[e] = jnp.broadcast_to(t_ref[0, 0, :, count + e:count + e + 1], (tokens, 128))

    acc[...] = jnp.zeros_like(acc)

    @pl.loop(0, count // 2)
    def _(pair):
        for c in range(0, half, COL):
            total = None
            for e in (2 * pair, 2 * pair + 1):
                wide = jnp.concatenate([gate[e]] * (COL // 128), axis=1)
                term = wide * dot32(pick[e], in_ref[0, e // experts, lax.rem(e, experts), 0, :, c:c + COL])
                total = term if total is None else total + term
            acc[:, c:c + COL] += total

    tile[...] = acc[...].astype(jnp.bfloat16)

    @pl.when(step < away)
    def _():
        put(step).start()

    @pl.when(step >= away)
    def _():
        keep(step).start()

    @pl.when(step == steps - 1)
    def _():
        keep(step).wait()

        @pl.loop(0, away)
        def _(s):
            send(s).wait()


def combine_call(side, cap, table, rows):
    _, _, tokens, width = table.shape
    turns, experts, half = rows.shape[1], rows.shape[2], rows.shape[5]
    count = width // 2
    dma = pltpu.SemaphoreType.DMA
    recv, _ = pl.pallas_call(
        functools.partial(combine_kernel, side, cap),
        grid=(side, 2),
        in_specs=[
            pl.BlockSpec((1, 1, tokens, width), lambda r, h: (h, (r + 1) % side, 0, 0)),
            pl.BlockSpec((1, turns, experts, 1, cap, half), lambda r, h: (h, 0, 0, (r + 1) % side, 0, 0)),
        ],
        out_specs=[pl.BlockSpec(memory_space=pl.ANY)] * 2,
        out_shape=[
            jax.ShapeDtypeStruct((2, side, tokens, half), jnp.bfloat16),
            jax.ShapeDtypeStruct((2 * side, tokens, half), jnp.bfloat16),
        ],
        scratch_shapes=[
            pltpu.VMEM((count, tokens, cap), jnp.bfloat16),
            pltpu.VMEM((count, tokens, 128), jnp.float32),
            pltpu.VMEM((tokens, half), jnp.float32),
            pltpu.VMEM((tokens, half), jnp.bfloat16),
            dma, dma((2 * side,)), dma((2 * side,)), dma,
        ],
        compiler_params=pltpu.CompilerParams(
            dimension_semantics=("arbitrary", "arbitrary"), vmem_limit_bytes=VMEM_LIMIT, has_side_effects=True),
        cost_estimate=pl.CostEstimate(flops=2 * tokens * rows.size, bytes_accessed=2 * rows.size, transcendentals=0),
        name="combine",
    )(table, rows)
    return recv


def routing(hidden, w_router, top_idx, keep_mask):
    experts = w_router.shape[1]
    tokens = hidden.shape[0]
    logits = jnp.dot(hidden, w_router, preferred_element_type=jnp.float32)
    prob = jax.nn.softmax(logits, axis=-1)
    chosen = (top_idx[:, :, None] == jnp.arange(experts)[None, None, :]) & (keep_mask[:, :, None] > 0)
    member = jnp.any(chosen, axis=1)
    lower = (jnp.arange(tokens)[:, None] >= jnp.arange(tokens)[None, :]).astype(jnp.bfloat16)
    count = jnp.dot(lower, member.astype(jnp.bfloat16), preferred_element_type=jnp.float32)
    rank = jnp.where(member, count - 1.0, -1.0)
    gate = jnp.where(member, ROUTE_SCALE * prob, 0.0)
    return rank, gate


def solution(mesh):
    groups = mesh.shape["ep"]
    side = math.isqrt(groups // CORES)
    tok_spec = P(("dp", "ep"), None)
    bank_spec = P("ep", None, None)
    rows_of = [[(y * side + x) * CORES + k for x in range(side)] for y in range(side) for k in range(CORES)]
    cols_of = [[(y * side + x) * CORES + k for y in range(side)] for x in range(side) for k in range(CORES)]

    def device_fn(hidden, w_router, w_gate, w_up, w_down, shared_gate, shared_up, shared_down, top_idx, keep_mask):
        tokens, top_k = top_idx.shape
        dim = hidden.shape[1]
        experts = w_router.shape[1]
        per_dev = w_gate.shape[0]
        cap = 8 * ((top_k * tokens + 4 * experts - 1) // (4 * experts))
        x_all = lax.all_gather(hidden, "ep", axis=0, tiled=True).reshape(groups, tokens, dim)
        rank, gate = routing(hidden, w_router, top_idx, keep_mask)
        table = lax.all_to_all(rank.T.reshape(groups, per_dev, tokens), "ep", 0, 0, tiled=True)
        here_x, here_y, _ = place(side)
        both = jnp.stack([rank, gate], axis=1).reshape(tokens, 2, side, side, CORES * per_dev)

        def exchange(blocks, peers, at):
            flat = blocks.reshape(side, tokens, 2 * side * CORES * per_dev)
            got = lax.all_to_all(flat, "ep", 0, 0, tiled=True, axis_index_groups=peers)
            return lax.dynamic_slice_in_dim(jnp.concatenate([got, got], axis=0), at, side, axis=0)

        by_x = exchange(both.transpose(3, 0, 1, 2, 4), rows_of, here_x)
        by_y = exchange(both.transpose(2, 0, 1, 3, 4), cols_of, here_y)
        pairs = jnp.stack([by_x, by_y])
        y = swiglu(hidden, shared_gate, shared_up, shared_down)
        x_all, y, pairs = lax.optimization_barrier((x_all, y, pairs))
        expert_rows = expert_call(side, cap, table, x_all, w_gate, w_up, w_down)
        sums = combine_call(side, cap, pairs, expert_rows).astype(jnp.float32)
        routed = jnp.concatenate([jnp.sum(sums[0], axis=0), jnp.sum(sums[1], axis=0)], axis=1)
        return (y + routed).astype(jnp.bfloat16)

    return jax.shard_map(device_fn, mesh=mesh, in_specs=(tok_spec, P(), bank_spec, bank_spec, bank_spec, P(), P(), P(), tok_spec, tok_spec), out_specs=tok_spec, check_vma=False)
```

```python
import functools
import math

import jax
import jax.numpy as jnp
from jax import lax
from jax.experimental import pallas as pl
from jax.experimental.pallas import tpu as pltpu
from jax.sharding import PartitionSpec as P

ROUTE_SCALE = 16.0
CORES = 2
COL = 256
VMEM_LIMIT = 63 * 1024 * 1024
MESH = pl.DeviceIdType.MESH


def swiglu(tok_rows, gate_w, up_w, down_w):
    h_gate = jnp.dot(tok_rows, gate_w, preferred_element_type=jnp.float32)
    h_up = jnp.dot(tok_rows, up_w, preferred_element_type=jnp.float32)
    act_rows = (jax.nn.silu(h_gate) * h_up).astype(jnp.bfloat16)
    return jnp.dot(act_rows, down_w, preferred_element_type=jnp.float32)


def dot32(a, b):
    return jnp.dot(a, b, preferred_element_type=jnp.float32)


def place(side):
    me = lax.axis_index("ep")
    return lax.rem(me // CORES, side), me // (CORES * side), lax.rem(me, CORES)


def device(side, x, y, k):
    return (lax.rem(y, side) * side + lax.rem(x, side)) * CORES + lax.rem(k, CORES)


def far_first(turn, side):
    g = lax.rem(turn + 1, side)
    return lax.rem(2 * g, side - 1) + (side - 1) * (g // (side - 1))


def pick_rows(rank, x, cap):
    hit = rank == lax.broadcasted_iota(jnp.int32, (cap, x.shape[0]), 0).astype(jnp.float32)
    return dot32(jnp.where(hit, 1.0, 0.0).astype(jnp.bfloat16), x).astype(jnp.bfloat16)


def fill_tail(tail, w1_ref, w3_ref):
    rest = tail.shape[1] // 2
    full = w1_ref.shape[2] - rest
    tail[:, :rest] = w1_ref[0, :, full:]
    tail[:, rest:] = w3_ref[0, :, full:]


def partial_kernel(cap, tab_ref, x_ref, w1_ref, w3_ref, o_ref, rows, tail):
    which, turn = pl.program_id(0), pl.program_id(1)
    per = x_ref.shape[0]
    full = w1_ref.shape[2] // COL * COL

    @pl.when(turn == 0)
    def _():
        fill_tail(tail, w1_ref, w3_ref)

    @pl.loop(0, per)
    def _(j):
        rank = tab_ref[turn * per + j, pl.ds(which, 1), :]
        rows[pl.ds(pl.multiple_of(j * cap, cap), cap), :] = pick_rows(rank, x_ref[j], cap)

    tok = rows[...]
    for c in range(0, full, COL):
        o_ref[0, :, :, c:c + COL] = dot32(tok, w1_ref[0, :, c:c + COL]).reshape(per, cap, COL)
        o_ref[0, :, :, full + c:full + c + COL] = dot32(tok, w3_ref[0, :, c:c + COL]).reshape(per, cap, COL)
    o_ref[0, :, :, 2 * full:] = dot32(tok, tail[...]).reshape(per, cap, tail.shape[1])


def partial_call(side, cap, tab, x_part, w1, w3):
    blocks, tokens, part = x_part.shape
    experts, _, ff = w1.shape
    once = pl.Buffered(1)
    return pl.pallas_call(
        functools.partial(partial_kernel, cap),
        grid=(experts, blocks // side),
        in_specs=[
            pl.BlockSpec(tab.shape, lambda e, t: (0, 0, 0), pipeline_mode=once),
            pl.BlockSpec((side, tokens, part), lambda e, t: (t, 0, 0)),
            pl.BlockSpec((1, part, ff), lambda e, t: (e, 0, 0), pipeline_mode=once),
            pl.BlockSpec((1, part, ff), lambda e, t: (e, 0, 0), pipeline_mode=once),
        ],
        out_specs=pl.BlockSpec((1, side, cap, 2 * ff), lambda e, t: (e, t, 0, 0)),
        out_shape=jax.ShapeDtypeStruct((experts, blocks, cap, 2 * ff), jnp.float32),
        scratch_shapes=[
            pltpu.VMEM((side * cap, part), jnp.bfloat16),
            pltpu.VMEM((part, 2 * (ff % COL)), jnp.bfloat16),
        ],
        compiler_params=pltpu.CompilerParams(dimension_semantics=("arbitrary", "arbitrary"), vmem_limit_bytes=VMEM_LIMIT),
        cost_estimate=pl.CostEstimate(
            flops=2 * experts * blocks * cap * part * (2 * ff + tokens), bytes_accessed=6 * x_part.size, transcendentals=0),
        name="partial_products",
    )(tab, x_part, w1, w3)


def expert_kernel(side, cap, tab_ref, x_ref, h_ref, w1_ref, w3_ref, w2_ref, recv, stage, xbuf, hbuf, rows, act, tail, tile,
                  x_sem, h_sem, stage_sem, send_a, recv_a, send_b, recv_b, self_sem):
    which, turn = pl.program_id(0), pl.program_id(1)
    turns = pl.num_programs(1)
    step = which * turns + turn
    steps = pl.num_programs(0) * turns
    ff = w1_ref.shape[2]
    full = ff // COL * COL
    rest = ff - full
    dim = w2_ref.shape[2]
    half = dim // 2
    x, y, k = place(side)

    def offsets(s):
        i = lax.rem(s, turns)
        return s // turns, far_first(i // CORES, side), lax.rem(i + 1, CORES)

    def fetch(s, j):
        _, dy, dc = offsets(s)
        return pltpu.make_async_copy(x_ref.at[device(side, x + j, y + dy, k + dc)], xbuf.at[j], x_sem.at[j])

    def fetch_h(s, j):
        e, dy, dc = offsets(s)
        return pltpu.make_async_copy(
            h_ref.at[e, device(side, x + j, y + dy, k + dc)], hbuf.at[pl.ds(j * cap, cap)], h_sem.at[j])

    def to_column(s):
        e, dy, dc = offsets(s)
        return pltpu.make_async_remote_copy(
            src_ref=stage.at[s, 0], dst_ref=recv.at[0, y * CORES + k, e], send_sem=send_a.at[s], recv_sem=recv_a.at[s],
            device_id={"ep": device(side, x, y + dy, k + dc)}, device_id_type=MESH)

    def to_row(s, dx):
        e, dy, dc = offsets(s)
        return pltpu.make_async_remote_copy(
            src_ref=stage.at[s, 1, dx], dst_ref=recv.at[1, x * CORES + k, e, dy], send_sem=send_b.at[s, dx], recv_sem=recv_b.at[s, dx],
            device_id={"ep": device(side, x + dx, y, k + dc)}, device_id_type=MESH)

    def keep_column(s):
        e, _, _ = offsets(s)
        return pltpu.make_async_copy(tile.at[0], recv.at[0, y * CORES + k, e], self_sem.at[0])

    def keep_row(s):
        e, dy, _ = offsets(s)
        return pltpu.make_async_copy(tile.at[1, 0], recv.at[1, x * CORES + k, e, dy], self_sem.at[1])

    def put(s):
        return pltpu.make_async_copy(tile, stage.at[s], stage_sem)

    def remotes(s, act_on):
        _, dy, dc = offsets(s)

        @pl.when((dy != 0) | (dc != 0))
        def _():
            act_on(to_column(s))

        @pl.when(dc != 0)
        def _():
            act_on(to_row(s, 0))

        for dx in (side // 2, *range(1, side // 2), *range(side // 2 + 1, side)):
            act_on(to_row(s, dx))

    def locals_(s, act_on):
        _, dy, dc = offsets(s)

        @pl.when((dy == 0) & (dc == 0))
        def _():
            act_on(keep_column(s))

        @pl.when(dc == 0)
        def _():
            act_on(keep_row(s))

    def flush(s):
        put(s).wait()
        locals_(s, lambda c: c.wait())
        remotes(s, lambda c: c.start())

    @pl.when(step == 0)
    def _():
        for j in range(side):
            fetch(0, j).start()
            fetch_h(0, j).start()

    if rest:
        @pl.when(turn == 0)
        def _():
            fill_tail(tail, w1_ref, w3_ref)

    _, now_y, now_c = offsets(step)

    @pl.loop(0, side)
    def _(j):
        fetch(step, j).wait()
        rank = tab_ref[device(side, x + j, y + now_y, k + now_c), pl.ds(which, 1), :]
        rows[pl.ds(pl.multiple_of(j * cap, cap), cap), :] = pick_rows(rank, xbuf[j], cap)

        @pl.when(step + 1 < steps)
        def _():
            fetch(step + 1, j).start()

    @pl.when(step > 0)
    def _():
        flush(step - 1)

    for j in range(side):
        fetch_h(step, j).wait()

    tok = rows[...]
    for c in range(0, full, COL):
        h_gate = hbuf[:, c:c + COL] + dot32(tok, w1_ref[0, :, c:c + COL])
        h_up = hbuf[:, full + c:full + c + COL] + dot32(tok, w3_ref[0, :, c:c + COL])
        act[:, c:c + COL] = (jax.nn.silu(h_gate) * h_up).astype(jnp.bfloat16)
    if rest:
        h_both = hbuf[:, 2 * full:] + dot32(tok, tail[...])
        act[:, full:] = (jax.nn.silu(h_both[:, :rest]) * h_both[:, rest:]).astype(jnp.bfloat16)

    @pl.when(step + 1 < steps)
    def _():
        for j in range(side):
            fetch_h(step + 1, j).start()

    a = act[...]
    for c in range(0, dim, COL):
        e = dot32(a, w2_ref[0, :, c:c + COL]).astype(jnp.bfloat16)
        at = c % half
        tile[c // half, :, :, at:at + COL] = e.reshape(side, cap, COL)

    put(step).start()
    locals_(step, lambda c: c.start())

    @pl.when(step == steps - 1)
    def _():
        flush(step)

        @pl.loop(0, steps)
        def _(s):
            remotes(s, lambda c: c.wait())


def expert_call(side, cap, tab, x_part, h_part, w1, w3, w2):
    blocks, tokens, part = x_part.shape
    experts, dim, ff = w1.shape
    once = pl.Buffered(1)
    turns = side * CORES
    steps = experts * turns
    rows = side * cap
    dma = pltpu.SemaphoreType.DMA
    recv, _ = pl.pallas_call(
        functools.partial(expert_kernel, side, cap),
        grid=(experts, turns),
        in_specs=[
            pl.BlockSpec(tab.shape, lambda e, t: (0, 0, 0), pipeline_mode=once),
            pl.BlockSpec(memory_space=pl.ANY),
            pl.BlockSpec(memory_space=pl.ANY),
            pl.BlockSpec((1, part, ff), lambda e, t: (e, dim // part - 1, 0)),
            pl.BlockSpec((1, part, ff), lambda e, t: (e, dim // part - 1, 0)),
            pl.BlockSpec((1, ff, dim), lambda e, t: (e, 0, 0), pipeline_mode=once),
        ],
        out_specs=[pl.BlockSpec(memory_space=pl.ANY)] * 2,
        out_shape=[
            jax.ShapeDtypeStruct((2, turns, experts, side, cap, dim // 2), jnp.bfloat16),
            jax.ShapeDtypeStruct((steps, 2, side, cap, dim // 2), jnp.bfloat16),
        ],
        scratch_shapes=[
            pltpu.VMEM((side, tokens, part), jnp.bfloat16),
            pltpu.VMEM((rows, 2 * ff), jnp.float32),
            pltpu.VMEM((rows, part), jnp.bfloat16),
            pltpu.VMEM((rows, ff), jnp.bfloat16),
            pltpu.VMEM((part, 2 * (ff % COL)), jnp.bfloat16),
            pltpu.VMEM((2, side, cap, dim // 2), jnp.bfloat16),
            dma((side,)), dma((side,)), dma, dma((steps,)), dma((steps,)), dma((steps, side)), dma((steps, side)), dma((2,)),
        ],
        compiler_params=pltpu.CompilerParams(
            dimension_semantics=("arbitrary", "arbitrary"), vmem_limit_bytes=VMEM_LIMIT, has_side_effects=True),
        cost_estimate=pl.CostEstimate(
            flops=2 * experts * blocks * cap * part * (4 * ff + tokens), bytes_accessed=8 * x_part.size, transcendentals=0),
        name="experts",
    )(tab, x_part, h_part, w1, w3, w2)
    return recv


def combine_kernel(side, cap, t_ref, in_ref, recv, stage, pick, gate, acc, tile, stage_sem, send_sem, recv_sem, self_sem):
    turn, part = pl.program_id(0), pl.program_id(1)
    step = turn * 2 + part
    steps = 2 * side
    tokens = t_ref.shape[2]
    count = t_ref.shape[3] // 2
    experts = in_ref.shape[2]
    half = in_ref.shape[5]
    x, y, k = place(side)

    def offsets(s):
        return far_first(s // 2, side), lax.rem(s, 2)

    def send(s):
        rel, h = offsets(s)
        return pltpu.make_async_remote_copy(
            src_ref=stage.at[s], dst_ref=recv.at[h, rel], send_sem=send_sem.at[s], recv_sem=recv_sem.at[s],
            device_id={"ep": device(side, x + rel * (1 - h), y + rel * h, k)}, device_id_type=MESH)

    def put(s):
        return pltpu.make_async_copy(tile, stage.at[s], stage_sem)

    def keep(s):
        rel, h = offsets(s)
        return pltpu.make_async_copy(tile, recv.at[h, rel], self_sem)

    away = steps - 2

    @pl.when((step > 0) & (step <= away))
    def _():
        put(step - 1).wait()
        send(step - 1).start()

    @pl.when(step > away)
    def _():
        keep(step - 1).wait()

    lanes = lax.broadcasted_iota(jnp.int32, (tokens, cap), 1).astype(jnp.float32)
    for e in range(count):
        pick[e] = jnp.where(t_ref[0, 0, :, e:e + 1] == lanes, 1.0, 0.0).astype(jnp.bfloat16)
        gate[e] = jnp.broadcast_to(t_ref[0, 0, :, count + e:count + e + 1], (tokens, 128))

    acc[...] = jnp.zeros_like(acc)

    @pl.loop(0, count // 2)
    def _(pair):
        for c in range(0, half, COL):
            total = None
            for e in (2 * pair, 2 * pair + 1):
                wide = jnp.concatenate([gate[e]] * (COL // 128), axis=1)
                term = wide * dot32(pick[e], in_ref[0, e // experts, lax.rem(e, experts), 0, :, c:c + COL])
                total = term if total is None else total + term
            acc[:, c:c + COL] += total

    tile[...] = acc[...].astype(jnp.bfloat16)

    @pl.when(step < away)
    def _():
        put(step).start()

    @pl.when(step >= away)
    def _():
        keep(step).start()

    @pl.when(step == steps - 1)
    def _():
        keep(step).wait()

        @pl.loop(0, away)
        def _(s):
            send(s).wait()


def combine_call(side, cap, table, rows):
    _, _, tokens, width = table.shape
    turns, experts, half = rows.shape[1], rows.shape[2], rows.shape[5]
    count = width // 2
    dma = pltpu.SemaphoreType.DMA
    recv, _ = pl.pallas_call(
        functools.partial(combine_kernel, side, cap),
        grid=(side, 2),
        in_specs=[
            pl.BlockSpec((1, 1, tokens, width), lambda r, h: (h, far_first(r, side), 0, 0)),
            pl.BlockSpec((1, turns, experts, 1, cap, half), lambda r, h: (h, 0, 0, far_first(r, side), 0, 0)),
        ],
        out_specs=[pl.BlockSpec(memory_space=pl.ANY)] * 2,
        out_shape=[
            jax.ShapeDtypeStruct((2, side, tokens, half), jnp.bfloat16),
            jax.ShapeDtypeStruct((2 * side, tokens, half), jnp.bfloat16),
        ],
        scratch_shapes=[
            pltpu.VMEM((count, tokens, cap), jnp.bfloat16),
            pltpu.VMEM((count, tokens, 128), jnp.float32),
            pltpu.VMEM((tokens, half), jnp.float32),
            pltpu.VMEM((tokens, half), jnp.bfloat16),
            dma, dma((2 * side,)), dma((2 * side,)), dma,
        ],
        compiler_params=pltpu.CompilerParams(
            dimension_semantics=("arbitrary", "arbitrary"), vmem_limit_bytes=VMEM_LIMIT, has_side_effects=True),
        cost_estimate=pl.CostEstimate(flops=2 * tokens * rows.size, bytes_accessed=2 * rows.size, transcendentals=0),
        name="combine",
    )(table, rows)
    return recv


def finish_kernel(sums_ref, y_ref, o_ref):
    _, sources, _, half = sums_ref.shape
    for part in range(2):
        cols = slice(part * half, (part + 1) * half)
        routed = sums_ref[part, 0].astype(jnp.float32)
        for i in range(1, sources):
            routed += sums_ref[part, i].astype(jnp.float32)
        o_ref[:, cols] = (y_ref[:, cols] + routed).astype(jnp.bfloat16)


def finish_call(sums, y):
    _, sources, tokens, half = sums.shape
    rows = tokens // 8
    return pl.pallas_call(
        finish_kernel,
        grid=(8,),
        in_specs=[
            pl.BlockSpec((2, sources, rows, half), lambda i: (0, 0, i, 0)),
            pl.BlockSpec((rows, 2 * half), lambda i: (i, 0)),
        ],
        out_specs=pl.BlockSpec((rows, 2 * half), lambda i: (i, 0)),
        out_shape=jax.ShapeDtypeStruct((tokens, 2 * half), jnp.bfloat16),
        compiler_params=pltpu.CompilerParams(dimension_semantics=("arbitrary",)),
        cost_estimate=pl.CostEstimate(flops=2 * sums.size, bytes_accessed=3 * sums.size, transcendentals=0),
        name="finish",
    )(sums, y)


def routing(hidden, w_router, top_idx, keep_mask):
    experts = w_router.shape[1]
    tokens = hidden.shape[0]
    logits = jnp.dot(hidden, w_router, preferred_element_type=jnp.float32)
    prob = jax.nn.softmax(logits, axis=-1)
    chosen = (top_idx[:, :, None] == jnp.arange(experts)[None, None, :]) & (keep_mask[:, :, None] > 0)
    member = jnp.any(chosen, axis=1)
    lower = (jnp.arange(tokens)[:, None] >= jnp.arange(tokens)[None, :]).astype(jnp.bfloat16)
    count = jnp.dot(lower, member.astype(jnp.bfloat16), preferred_element_type=jnp.float32)
    rank = jnp.where(member, count - 1.0, -1.0)
    gate = jnp.where(member, ROUTE_SCALE * prob, 0.0)
    return rank, gate


def solution(mesh):
    groups = mesh.shape["ep"]
    side = math.isqrt(groups // CORES)
    tok_spec = P(("dp", "ep"), None)
    bank_spec = P("ep", None, None)
    rows_of = [[(y * side + x) * CORES + k for x in range(side)] for y in range(side) for k in range(CORES)]
    cols_of = [[(y * side + x) * CORES + k for y in range(side)] for x in range(side) for k in range(CORES)]

    def device_fn(hidden, w_router, w_gate, w_up, w_down, shared_gate, shared_up, shared_down, top_idx, keep_mask):
        tokens, top_k = top_idx.shape
        dim = hidden.shape[1]
        experts = w_router.shape[1]
        per_dev = w_gate.shape[0]
        cap = 8 * ((top_k * tokens + 4 * experts - 1) // (4 * experts))
        half = dim // 2
        x_low, x_high = (
            lax.all_gather(h, "ep", axis=0, tiled=True).reshape(groups, tokens, half) for h in (hidden[:, :half], hidden[:, half:]))
        rank, gate = routing(hidden, w_router, top_idx, keep_mask)
        table = lax.all_to_all(rank.T.reshape(groups, per_dev, tokens), "ep", 0, 0, tiled=True)
        here_x, here_y, _ = place(side)
        both = jnp.stack([rank, gate], axis=1).reshape(tokens, 2, side, side, CORES * per_dev)

        def exchange(blocks, peers, at):
            flat = blocks.reshape(side, tokens, 2 * side * CORES * per_dev)
            got = lax.all_to_all(flat, "ep", 0, 0, tiled=True, axis_index_groups=peers)
            return lax.dynamic_slice_in_dim(jnp.concatenate([got, got], axis=0), at, side, axis=0)

        by_x = exchange(both.transpose(3, 0, 1, 2, 4), rows_of, here_x)
        by_y = exchange(both.transpose(2, 0, 1, 3, 4), cols_of, here_y)
        pairs = jnp.stack([by_x, by_y])
        y = swiglu(hidden, shared_gate, shared_up, shared_down)
        partial = partial_call(side, cap, table, x_low, w_gate, w_up)
        partial, x_high, y, pairs = lax.optimization_barrier((partial, x_high, y, pairs))
        expert_rows = expert_call(side, cap, table, x_high, partial, w_gate, w_up, w_down)
        return finish_call(combine_call(side, cap, pairs, expert_rows), y)

    return jax.shard_map(device_fn, mesh=mesh, in_specs=(tok_spec, P(), bank_spec, bank_spec, bank_spec, P(), P(), P(), tok_spec, tok_spec), out_specs=tok_spec, check_vma=False)
```
